32 devices in a mesh: dp: 1, sp: 32 (over x, y, z, core).
Axes of the slice: x: 2, y: 2, z: 4, core: 2. Of those that a mesh axis runs over, the one named last changes fastest.
Arguments:
- x: bfloat16 [4096, 4096], P(('dp', 'sp'))
- gain: bfloat16 [4096], replicated
- wq: bfloat16 [4096, 4096], replicated
- wk: bfloat16 [4096, 256], replicated
- wv: bfloat16 [4096, 256], replicated
- wo: bfloat16 [4096, 4096], replicated
Outputs:
- output: bfloat16 [4096, 4096], P(('dp', 'sp'))
All inputs are finite; a program needn't handle non-finite values.
Results may differ from the reference program's by a relative error of at most 0.012.
Values are sent between devices in bfloat16 or wider.
A program may use at most 2 GiB of HBM per device.

```python
import jax
import jax.numpy as jnp
from jax import lax

ROWS = 4096
D = 4096
HEADS = 16
KV_HEADS = 1
HEAD = 256
THETA = 10000


def setup_inputs(seed: int = 0, part: int = 0) -> dict:
    kx, kn, kq, kk, kv, ko = jax.random.split(jax.random.key(seed), 6)

    def weights(key, rows, columns):
        return jax.random.normal(key, (rows, columns), jnp.float32) * rows**-0.5

    drawn = {
        "x": jax.random.normal(jax.random.fold_in(kx, part), (ROWS, D), jnp.float32),
        "gain": 1 + 0.1 * jax.random.normal(kn, (D,), jnp.float32),
        "wq": 2 * weights(kq, D, HEADS * HEAD),
        "wk": 2 * weights(kk, D, KV_HEADS * HEAD),
        "wv": 4 * weights(kv, D, KV_HEADS * HEAD),
        "wo": weights(ko, HEADS * HEAD, D),
    }
    return {k: v.astype(jnp.bfloat16) for k, v in drawn.items()}


def normed(x, gain):
    wide = x.astype(jnp.float32)
    scale = lax.rsqrt(jnp.mean(wide * wide, -1, keepdims=True) + 1e-6)
    return (wide * scale * gain.astype(jnp.float32)).astype(jnp.bfloat16)


def turned(t, place, theta):
    half = t.shape[-1] // 2
    angle = place.astype(jnp.float32)[:, None] * theta ** (-jnp.arange(half, dtype=jnp.float32) / half)
    cos, sin = jnp.cos(angle)[:, None], jnp.sin(angle)[:, None]
    a, b = t[..., :half].astype(jnp.float32), t[..., half:].astype(jnp.float32)
    return jnp.concatenate([a * cos - b * sin, b * cos + a * sin], -1).astype(jnp.bfloat16)


def matmul(a, w):
    return jnp.dot(a, w, preferred_element_type=jnp.float32).astype(jnp.bfloat16)


def einsum(form, a, b):
    return jnp.einsum(form, a.astype(jnp.float32), b.astype(jnp.float32))


def attention(q, k, v):
    scores = einsum("tgsd,ugd->gstu", q, k) * q.shape[-1] ** -0.5
    token = jnp.arange(q.shape[0])
    scores = jnp.where(token[:, None] >= token, scores, -jnp.inf)
    weights = jax.nn.softmax(scores, -1).astype(jnp.bfloat16)
    return einsum("gstu,ugd->tgsd", weights, v).astype(jnp.bfloat16)


def reference(x, gain, wq, wk, wv, wo):
    a, place = normed(x, gain), jnp.arange(ROWS)
    q = turned(matmul(a, wq).reshape(ROWS, HEADS, HEAD), place, THETA).reshape(ROWS, KV_HEADS, -1, HEAD)
    k = turned(matmul(a, wk).reshape(ROWS, KV_HEADS, HEAD), place, THETA)
    v = matmul(a, wv).reshape(ROWS, KV_HEADS, HEAD)
    seen = attention(q, k, v).reshape(ROWS, HEADS * HEAD)
    return (x.astype(jnp.float32) + jnp.dot(seen, wo, preferred_element_type=jnp.float32)).astype(jnp.bfloat16)
```

```python
import functools

import jax
import jax.numpy as jnp
import numpy as np
from jax import lax
from jax.experimental import pallas as pl
from jax.experimental.pallas import tpu as pltpu
from jax.sharding import PartitionSpec as P

HEAD = 256
HALF = 128
HEADS = 16
D = 4096
OWN = 128
THETA = 10000
LOG2E = 1.4426950408889634
E = HEAD**-0.5 * LOG2E
HIDDEN = -2e30
SLOTS = 22
CHUNKS = 34
STRIPS = 8
SENDS = 62
MESH = pl.DeviceIdType.MESH


def _dot(a, b):
    return jnp.dot(a, b, preferred_element_type=jnp.float32)


def _kernel(x_hbm, gain_hbm, freq_hbm, wk, wv, wq, wo, out, x_s, gain_s, freq_s, a_s, w_s, k_s, v_s, q_s, seen_s, mix_s, top_s, cos_s,
            sin_s, in_sem, w_sem, send_sem, k_sem, v_sem, out_sem):
    me = lax.axis_index("sp")
    core = lax.rem(me, 2)
    chip = lax.div(me, 2)
    z = lax.rem(chip, 4)
    line = lax.div(chip, 4)
    y = lax.rem(line, 2)
    x = lax.div(line, 2)

    lines = {"o": line, "y": 2 * x + 1 - y, "x": 2 * (1 - x) + y, "d": 2 * (1 - x) + 1 - y}
    near, two, far = z + 1 - 2 * lax.rem(z, 2), lax.rem(z + 2, 4), 3 - z
    mid = lax.rem(lax.div(z + 1, 2), 2)
    places = [z, near, two + mid * (far - two), far + mid * (two - far)]

    def block(name, at, c=None):
        return (lines[name] * 4 + places[at]) * 2 + (core if c is None else c)

    other = me + 1 - 2 * core
    peers = {"p": other, "y": block("y", 0), "x": block("x", 0), 1: block("o", 1), 2: block("o", 2), 3: block("o", 3)}

    def copy(kind, b, to, n):
        ref = (k_s if kind == "k" else v_s).at[b]
        return pltpu.make_async_remote_copy(src_ref=ref, dst_ref=ref, send_sem=send_sem.at[n],
                                            recv_sem=(k_sem if kind == "k" else v_sem).at[b],
                                            device_id=(0, to), device_id_type=MESH)

    sent = [0]

    def send(kind, b, *to):
        for t in to:
            copy(kind, b, peers[t], sent[0]).start()
            sent[0] += 1

    def arrived(kind, b):
        copy(kind, b, other, 0).wait_recv()

    def relay(kind, name, at, *to):
        b = block(name, at)
        arrived(kind, b)
        send(kind, b, *to)

    def fetch(c):
        src = wk if c == 0 else wv if c == 1 else wq.at[:, pl.ds((c - 2) * 256, 256)] if c < 18 else wo.at[:, pl.ds((c - 18) * 256, 256)]
        return pltpu.make_async_copy(src, w_s.at[c % SLOTS], w_sem.at[c % SLOTS])

    def fetch_out(i):
        slot = lax.rem(i + 18, SLOTS)
        return pltpu.make_async_copy(wo.at[:, pl.ds(pl.multiple_of(i * 256, 256), 256)], w_s.at[slot], w_sem.at[slot])

    def landed(slot):
        pltpu.make_async_copy(wk, w_s.at[slot], w_sem.at[slot]).wait()

    x_copy = pltpu.make_async_copy(x_hbm, x_s, in_sem.at[0])
    gain_copy = pltpu.make_async_copy(gain_hbm, gain_s, in_sem.at[1])
    freq_copy = pltpu.make_async_copy(freq_hbm, freq_s, in_sem.at[2])
    x_copy.start()
    gain_copy.start()
    freq_copy.start()
    for c in range(SLOTS):
        fetch(c).start()

    barrier = pltpu.get_barrier_semaphore()
    for t in peers.values():
        pl.semaphore_signal(barrier, inc=1, device_id=(0, t), device_id_type=MESH)

    freq_copy.wait()
    angle = (me * OWN + lax.broadcasted_iota(jnp.int32, (OWN, HALF), 0)).astype(jnp.float32) * freq_s[0:1, :]
    cos_s[...] = jnp.cos(angle)
    sin_s[...] = jnp.sin(angle)

    x_copy.wait()
    gain_copy.wait()

    def norm(r, _):
        rows = pl.ds(pl.multiple_of(r * 16, 16), 16)
        wide = x_s[rows, :].astype(jnp.float32)
        scale = lax.rsqrt(jnp.mean(wide * wide, -1, keepdims=True) + 1e-6)
        a_s[rows, :] = (wide * scale * gain_s[0:1, :].astype(jnp.float32)).astype(jnp.bfloat16)

    lax.fori_loop(0, OWN // 16, norm, None)

    def projected(slot):
        return _dot(a_s[...], w_s[slot]).astype(jnp.bfloat16).astype(jnp.float32)

    def turned(t):
        a, b = t[:, :HALF], t[:, HALF:]
        cos, sin = cos_s[...], sin_s[...]
        return a * cos - b * sin, b * cos + a * sin

    landed(0)
    first, second = turned(projected(0))
    k_s[me, :, :HALF] = first.astype(jnp.bfloat16)
    k_s[me, :, HALF:] = second.astype(jnp.bfloat16)
    landed(1)
    v_s[me] = projected(1).T.astype(jnp.bfloat16)
    fetch(SLOTS).start()
    fetch(SLOTS + 1).start()

    pl.semaphore_wait(barrier, len(peers))
    send("k", me, 1, "y")
    send("v", me, 1, "x")
    send("k", me, "p", "x", 2)
    send("v", me, "p", "y", 2)
    send("k", me, 3)
    send("v", me, 3)

    def own_line(at):
        relay("k", "o", at, "y", "x", "p")
        relay("v", "o", at, "x", "y", "p")

    def across(at):
        relay("k", "y", at, "x", "p")
        relay("v", "x", at, "y", "p")

    def back(at):
        relay("v", "y", at, "p")
        relay("k", "x", at, "p")

    def corner(at):
        relay("k", "d", at, "p")
        relay("v", "d", at, "p")

    def from_other(*which):
        for name, at in which:
            b = block(name, at, 1 - core)
            arrived("k", b)
            arrived("v", b)

    def timed(step, events):
        for at, calls in events.items():
            @pl.when(step == at)
            def _(calls=calls):
                for f, *args in calls:
                    f(*args)

    def query(j, _):
        slot = j + 2
        landed(slot)
        first, second = turned(projected(slot))
        q_s[j, :HALF, :] = first.T.astype(jnp.bfloat16)
        q_s[j, HALF:, :] = second.T.astype(jnp.bfloat16)

        @pl.when(j < CHUNKS - SLOTS - 2)
        def _():
            fetch_out(j + SLOTS + 2 - 18).start()

        timed(j, {
            4: [(across, 0)],
            7: [(own_line, 1), (back, 0)],
            10: [(corner, 0)],
            12: [(across, 1)],
            14: [(back, 1)],
            15: [(own_line, 2), (from_other, ("o", 0), ("o", 1))],
        })

    lax.fori_loop(0, HEADS, query, None)

    def attend(start, masked):
        keys = k_s[pl.ds(start, 4)].reshape(512, HEAD)
        values = jnp.concatenate([v_s[start + i] for i in range(4)], axis=1)
        values = jnp.concatenate([values, jnp.ones((8, 512), jnp.bfloat16)], axis=0)

        def scores(i):
            return _dot(keys, jnp.concatenate([q_s[2 * i], q_s[2 * i + 1]], axis=1))

        if masked:
            place = lax.rem(z, 2) * 256 + core * OWN + lax.rem(lax.broadcasted_iota(jnp.int32, (512, 256), 1), OWN)
            ok = lax.broadcasted_iota(jnp.int32, (512, 256), 0) <= place
        s = scores(0)
        for i in range(STRIPS):
            then = scores(i + 1) if i + 1 < STRIPS else None
            if masked:
                s = jnp.where(ok, s, HIDDEN)
                top = s.max(axis=0, keepdims=True)
                p = jnp.exp2((s - top) * E).astype(jnp.bfloat16)
                mix_s[i] = _dot(values, p)
            else:
                old = top_s[i : i + 1, :]
                top = jnp.maximum(old, s.max(axis=0, keepdims=True))
                p = jnp.exp2((s - top) * E).astype(jnp.bfloat16)
                mix_s[i] = mix_s[i] * jnp.exp2((old - top) * E) + _dot(values, p)
            top_s[i : i + 1, :] = top
            s = then

    half = lax.div(z, 2)
    attend(line * 8 + half * 4, True)

    def step(h, _):
        near_half = h < 3
        turn = lax.rem(h + 1, 4)
        dx, dy = lax.div(turn, 2), lax.rem(turn, 2)
        lx, ly = x + dx * (1 - 2 * x), y + dy * (1 - 2 * y)
        hz = jnp.where(near_half, half, 1 - half)
        timed(h, {
            0: [(corner, 1), (from_other, ("y", 0), ("y", 1))],
            1: [(own_line, 3), (across, 2), (from_other, ("x", 0), ("x", 1))],
            2: [(back, 2), (from_other, ("d", 0), ("d", 1))],
            3: [(across, 3), (from_other, ("o", 2), ("o", 3))],
            4: [(back, 3), (corner, 2), (from_other, ("y", 2), ("y", 3))],
            5: [(corner, 3), (from_other, ("x", 2), ("x", 3))],
            6: [(from_other, ("d", 2), ("d", 3))],
        })
        block_of = (2 * lx + ly) * 2 + hz
        @pl.when(block_of < line * 2 + half)
        def _():
            attend(block_of * 4, False)

    lax.fori_loop(0, 7, step, None)

    for i in range(STRIPS):
        done = mix_s[i, :HEAD, :] * (1 / mix_s[i, HEAD : HEAD + 1, :])
        for n in range(2):
            seen_s[:, (2 * i + n) * HEAD : (2 * i + n + 1) * HEAD] = done[:, n * OWN : (n + 1) * OWN].T.astype(jnp.bfloat16)

    def put(i):
        cols = pl.ds(pl.multiple_of(i * 512, 512), 512)
        return pltpu.make_async_copy(a_s.at[:, cols], out.at[:, cols], out_sem.at[i])

    def project(i, _):
        for n in range(2):
            slot = lax.rem(2 * i + n + 18, SLOTS)
            landed(slot)
        for n in range(2):
            slot = lax.rem(2 * i + n + 18, SLOTS)
            cols = pl.ds(pl.multiple_of((2 * i + n) * 256, 256), 256)
            a_s[:, cols] = (x_s[:, cols].astype(jnp.float32) + _dot(seen_s[...], w_s[slot])).astype(jnp.bfloat16)
        put(i).start()

    lax.fori_loop(0, 8, project, None)
    for i in range(8):
        put(i).wait()
    assert sent[0] == SENDS

    def drain(n, _):
        copy("k", me, other, n).wait_send()

    lax.fori_loop(0, SENDS, drain, None)


def solution(mesh):
    freq = np.float32(THETA) ** (-np.arange(HALF, dtype=np.float32) / np.float32(HALF))

    def step(x, gain, wq, wk, wv, wo):
        bf16, f32 = jnp.bfloat16, jnp.float32
        return pl.pallas_call(
            _kernel,
            out_shape=jax.ShapeDtypeStruct((OWN, D), bf16),
            in_specs=[pl.BlockSpec(memory_space=pl.ANY)] * 7,
            out_specs=pl.BlockSpec(memory_space=pl.ANY),
            scratch_shapes=[
                pltpu.VMEM((OWN, D), bf16),
                pltpu.VMEM((1, D), bf16),
                pltpu.VMEM((1, HALF), f32),
                pltpu.VMEM((OWN, D), bf16),
                pltpu.VMEM((SLOTS, D, 256), bf16),
                pltpu.VMEM((32, OWN, HEAD), bf16),
                pltpu.VMEM((32, HEAD, OWN), bf16),
                pltpu.VMEM((HEADS, HEAD, OWN), bf16),
                pltpu.VMEM((OWN, D), bf16),
                pltpu.VMEM((STRIPS, HEAD + 8, 256), f32),
                pltpu.VMEM((STRIPS, 256), f32),
                pltpu.VMEM((OWN, HALF), f32),
                pltpu.VMEM((OWN, HALF), f32),
                pltpu.SemaphoreType.DMA((3,)),
                pltpu.SemaphoreType.DMA((SLOTS,)),
                pltpu.SemaphoreType.DMA((SENDS,)),
                pltpu.SemaphoreType.DMA((32,)),
                pltpu.SemaphoreType.DMA((32,)),
                pltpu.SemaphoreType.DMA((8,)),
            ],
            compiler_params=pltpu.CompilerParams(collective_id=0, has_side_effects=True, vmem_limit_bytes=67043328),
        )(x, gain[None], jnp.asarray(freq)[None], wk, wv, wq, wo)

    tokens, whole = P(("dp", "sp"), None), P(None, None)
    return jax.shard_map(
        step,
        mesh=mesh,
        in_specs=(tokens, P(None), whole, whole, whole, whole),
        out_specs=tokens,
        check_vma=False,
    )
```

```python
import functools

import jax
import jax.numpy as jnp
import numpy as np
from jax import lax
from jax.experimental import pallas as pl
from jax.experimental.pallas import tpu as pltpu
from jax.sharding import PartitionSpec as P

HEAD = 256
HALF = 128
HEADS = 16
D = 4096
OWN = 128
THETA = 10000
LOG2E = 1.4426950408889634
E = HEAD**-0.5 * LOG2E
HIDDEN = -2e30
SLOTS = 22
CHUNKS = 34
STRIPS = 8
SENDS = 62
MESH = pl.DeviceIdType.MESH


def _dot(a, b):
    return jnp.dot(a, b, preferred_element_type=jnp.float32)


def _kernel(x_hbm, gain_hbm, turn_hbm, base_hbm, wk, wv, wq, wo, out, x_s, gain_s, turn_s, base_s, a_s, w_s, k_s, v_s, q_s, seen_s, mix_s, top_s, cos_s,
            sin_s, in_sem, w_sem, send_sem, k_sem, v_sem, out_sem):
    me = lax.axis_index("sp")
    core = lax.rem(me, 2)
    chip = lax.div(me, 2)
    z = lax.rem(chip, 4)
    line = lax.div(chip, 4)
    y = lax.rem(line, 2)
    x = lax.div(line, 2)

    lines = {"o": line, "y": 2 * x + 1 - y, "x": 2 * (1 - x) + y, "d": 2 * (1 - x) + 1 - y}
    near, two, far = z + 1 - 2 * lax.rem(z, 2), lax.rem(z + 2, 4), 3 - z
    mid = lax.rem(lax.div(z + 1, 2), 2)
    places = [z, near, two + mid * (far - two), far + mid * (two - far)]

    def block(name, at, c=None):
        return (lines[name] * 4 + places[at]) * 2 + (core if c is None else c)

    other = me + 1 - 2 * core
    peers = {"p": other, "y": block("y", 0), "x": block("x", 0), 1: block("o", 1), 2: block("o", 2), 3: block("o", 3)}

    def copy(kind, b, to, n):
        ref = (k_s if kind == "k" else v_s).at[b]
        return pltpu.make_async_remote_copy(src_ref=ref, dst_ref=ref, send_sem=send_sem.at[n % 2],
                                            recv_sem=(k_sem if kind == "k" else v_sem).at[b],
                                            device_id=(0, to), device_id_type=MESH)

    sent = [0]

    def send(kind, b, *to):
        for t in to:
            copy(kind, b, peers[t], sent[0]).start()
            sent[0] += 1

    def arrived(kind, b):
        copy(kind, b, other, 0).wait_recv()

    def relay(kind, name, at, *to):
        b = block(name, at)
        arrived(kind, b)
        send(kind, b, *to)

    def fetch(c):
        src = wk if c == 0 else wv if c == 1 else wq.at[:, pl.ds((c - 2) * 256, 256)] if c < 18 else wo.at[:, pl.ds((c - 18) * 256, 256)]
        return pltpu.make_async_copy(src, w_s.at[c % SLOTS], w_sem.at[c % SLOTS])

    def landed(slot):
        pltpu.make_async_copy(wk, w_s.at[slot], w_sem.at[slot]).wait()

    x_copy = pltpu.make_async_copy(x_hbm, x_s, in_sem.at[0])
    gain_copy = pltpu.make_async_copy(gain_hbm, gain_s, in_sem.at[1])
    turn_copy = pltpu.make_async_copy(turn_hbm, turn_s, in_sem.at[2])
    base_copy = pltpu.make_async_copy(base_hbm.at[me], base_s, in_sem.at[3])
    x_copy.start()
    gain_copy.start()
    turn_copy.start()
    base_copy.start()
    for c in range(SLOTS):
        fetch(c).start()

    barrier = pltpu.get_barrier_semaphore()
    for t in peers.values():
        pl.semaphore_signal(barrier, inc=1, device_id=(0, t), device_id_type=MESH)

    turn_copy.wait()
    base_copy.wait()
    near_cos, near_sin, far_cos, far_sin = turn_s[0], turn_s[1], base_s[0:1, :], base_s[1:2, :]
    cos_s[...] = near_cos * far_cos - near_sin * far_sin
    sin_s[...] = near_sin * far_cos + near_cos * far_sin

    x_copy.wait()
    gain_copy.wait()

    gain = gain_s[...].reshape(1, D).astype(jnp.float32)
    for r in range(OWN // 16):
        rows = slice(r * 16, (r + 1) * 16)
        wide = x_s[rows, :].astype(jnp.float32)
        scale = lax.rsqrt(jnp.mean(wide * wide, -1, keepdims=True) + 1e-6)
        a_s[rows, :] = (wide * scale * gain).astype(jnp.bfloat16)

    def projected(slot):
        return _dot(a_s[...], w_s[slot]).astype(jnp.bfloat16).astype(jnp.float32)

    def turned(t):
        a, b = t[:, :HALF], t[:, HALF:]
        cos, sin = cos_s[...], sin_s[...]
        return a * cos - b * sin, b * cos + a * sin

    landed(0)
    landed(1)
    first, second = turned(projected(0))
    values = projected(1)
    k_s[me, :, :HALF] = first.astype(jnp.bfloat16)
    k_s[me, :, HALF:] = second.astype(jnp.bfloat16)
    v_s[me] = values.T.astype(jnp.bfloat16)
    fetch(SLOTS).start()
    fetch(SLOTS + 1).start()

    pl.semaphore_wait(barrier, len(peers))
    send("k", me, 1, "y")
    send("v", me, 1, "x")
    send("k", me, "p", "x", 2)
    send("v", me, "p", "y", 2)
    send("k", me, 3)
    send("v", me, 3)

    def own_line(at):
        relay("k", "o", at, "y", "x", "p")
        relay("v", "o", at, "x", "y", "p")

    def across(at):
        relay("k", "y", at, "x", "p")
        relay("v", "x", at, "y", "p")

    def back(at):
        relay("v", "y", at, "p")
        relay("k", "x", at, "p")

    def corner(at):
        relay("k", "d", at, "p")
        relay("v", "d", at, "p")

    def from_other(*which):
        for name, at in which:
            b = block(name, at, 1 - core)
            arrived("k", b)
            arrived("v", b)

    events = {
        2: [(across, 0)],
        3: [(own_line, 1), (back, 0)],
        4: [(corner, 0)],
        5: [(across, 1)],
        6: [(back, 1)],
        7: [(own_line, 2), (from_other, ("o", 0), ("o", 1))],
    }
    for j in range(0, HEADS, 2):
        landed(j + 2)
        landed(j + 3)
        both = [projected(j + 2), projected(j + 3)]
        for n in range(2):
            first, second = turned(both[n])
            q_s[j + n, :HALF, :] = first.T.astype(jnp.bfloat16)
            q_s[j + n, HALF:, :] = second.T.astype(jnp.bfloat16)
        for c in (j + 2 + SLOTS, j + 3 + SLOTS):
            if c < CHUNKS:
                fetch(c).start()
        for f, *args in events.get(j // 2, ()):
            f(*args)

    def attend(start, masked):
        keys = k_s[pl.ds(start, 4)].reshape(512, HEAD)
        values = jnp.concatenate([v_s[start + i] for i in range(4)], axis=1)
        values = jnp.concatenate([values, jnp.ones((8, 512), jnp.bfloat16)], axis=0)

        def scores(i):
            return _dot(keys, jnp.concatenate([q_s[2 * i], q_s[2 * i + 1]], axis=1))

        if masked:
            place = lax.rem(z, 2) * 256 + core * OWN + lax.rem(lax.broadcasted_iota(jnp.int32, (512, 256), 1), OWN)
            ok = lax.broadcasted_iota(jnp.int32, (512, 256), 0) <= place
        s = scores(0)
        for i in range(STRIPS):
            then = scores(i + 1) if i + 1 < STRIPS else None
            if masked:
                s = jnp.where(ok, s, HIDDEN)
                top = s.max(axis=0, keepdims=True)
                p = jnp.exp2((s - top) * E).astype(jnp.bfloat16)
                mix_s[i] = _dot(values, p)
            else:
                old = top_s[i : i + 1, :]
                top = jnp.maximum(old, s.max(axis=0, keepdims=True))
                p = jnp.exp2((s - top) * E).astype(jnp.bfloat16)
                mix_s[i] = mix_s[i] * jnp.exp2((old - top) * E) + _dot(values, p)
            top_s[i : i + 1, :] = top
            s = then

    half = lax.div(z, 2)
    attend(line * 8 + half * 4, True)

    for name, h, calls in (
        ("y", half, [(corner, 1), (from_other, ("y", 0), ("y", 1))]),
        ("x", half, [(own_line, 3), (across, 2), (from_other, ("x", 0), ("x", 1))]),
        ("d", half, [(back, 2), (from_other, ("d", 0), ("d", 1))]),
        ("o", 1 - half, [(across, 3), (from_other, ("o", 2), ("o", 3))]),
        ("y", 1 - half, [(back, 3), (corner, 2), (from_other, ("y", 2), ("y", 3))]),
        ("x", 1 - half, [(corner, 3), (from_other, ("x", 2), ("x", 3))]),
        ("d", 1 - half, [(from_other, ("d", 2), ("d", 3))]),
    ):
        for f, *args in calls:
            f(*args)
        start = lines[name] * 2 + h

        @pl.when(start < line * 2 + half)
        def _(start=start):
            attend(start * 4, False)

    for i in range(STRIPS):
        done = mix_s[i, :HEAD, :] * (1 / mix_s[i, HEAD : HEAD + 1, :])
        for n in range(2):
            seen_s[:, (2 * i + n) * HEAD : (2 * i + n + 1) * HEAD] = done[:, n * OWN : (n + 1) * OWN].T.astype(jnp.bfloat16)

    def put(i):
        cols = pl.ds(pl.multiple_of(i * 512, 512), 512)
        return pltpu.make_async_copy(a_s.at[:, cols], out.at[:, cols], out_sem.at[i])

    def project(i, _):
        for n in range(2):
            slot = lax.rem(2 * i + n + 18, SLOTS)
            landed(slot)
        for n in range(2):
            slot = lax.rem(2 * i + n + 18, SLOTS)
            cols = pl.ds(pl.multiple_of((2 * i + n) * 256, 256), 256)
            a_s[:, cols] = (x_s[:, cols].astype(jnp.float32) + _dot(seen_s[...], w_s[slot])).astype(jnp.bfloat16)
        put(i).start()

    lax.fori_loop(0, 8, project, None)
    assert sent[0] == SENDS
    for n in range(2):
        ref = k_s.at[pl.ds(0, SENDS // 2)]
        pltpu.make_async_copy(ref, ref, send_sem.at[n]).wait()
    for i in range(8):
        put(i).wait()


def solution(mesh):
    angle = np.float64(THETA) ** (-np.arange(HALF) / HALF)
    near, far = np.arange(OWN)[:, None] * angle, np.arange(32)[:, None] * OWN * angle
    near = np.stack([np.cos(near), np.sin(near)]).astype(np.float32)
    far = np.stack([np.cos(far), np.sin(far)], 1).astype(np.float32)

    def step(x, gain, wq, wk, wv, wo):
        bf16, f32 = jnp.bfloat16, jnp.float32
        return pl.pallas_call(
            _kernel,
            out_shape=jax.ShapeDtypeStruct((OWN, D), bf16),
            in_specs=[pl.BlockSpec(memory_space=pl.ANY)] * 8,
            out_specs=pl.BlockSpec(memory_space=pl.ANY),
            scratch_shapes=[
                pltpu.VMEM((OWN, D), bf16),
                pltpu.VMEM((D,), bf16),
                pltpu.VMEM((2, OWN, HALF), f32),
                pltpu.VMEM((2, HALF), f32),
                pltpu.VMEM((OWN, D), bf16),
                pltpu.VMEM((SLOTS, D, 256), bf16),
                pltpu.VMEM((32, OWN, HEAD), bf16),
                pltpu.VMEM((32, HEAD, OWN), bf16),
                pltpu.VMEM((HEADS, HEAD, OWN), bf16),
                pltpu.VMEM((OWN, D), bf16),
                pltpu.VMEM((STRIPS, HEAD + 8, 256), f32),
                pltpu.VMEM((STRIPS, 256), f32),
                pltpu.VMEM((OWN, HALF), f32),
                pltpu.VMEM((OWN, HALF), f32),
                pltpu.SemaphoreType.DMA((4,)),
                pltpu.SemaphoreType.DMA((SLOTS,)),
                pltpu.SemaphoreType.DMA((2,)),
                pltpu.SemaphoreType.DMA((32,)),
                pltpu.SemaphoreType.DMA((32,)),
                pltpu.SemaphoreType.DMA((8,)),
            ],
            compiler_params=pltpu.CompilerParams(collective_id=0, has_side_effects=True, vmem_limit_bytes=67043328),
        )(x, gain, jnp.asarray(near), jnp.asarray(far), wk, wv, wq, wo)

    tokens, whole = P(("dp", "sp"), None), P(None, None)
    return jax.shard_map(
        step,
        mesh=mesh,
        in_specs=(tokens, P(None), whole, whole, whole, whole),
        out_specs=tokens,
        check_vma=False,
    )
```

```python
import functools

import jax
import jax.numpy as jnp
import numpy as np
from jax import lax
from jax.experimental import pallas as pl
from jax.experimental.pallas import tpu as pltpu
from jax.sharding import PartitionSpec as P

HEAD = 256
HALF = 128
HEADS = 16
D = 4096
OWN = 128
THETA = 10000
LOG2E = 1.4426950408889634
E = HEAD**-0.5 * LOG2E
HIDDEN = -2e30
SLOTS = 22
CHUNKS = 34
DEPTH = 4
STRIPS = 8
SENDS = 62
MESH = pl.DeviceIdType.MESH


def _dot(a, b):
    return jnp.dot(a, b, preferred_element_type=jnp.float32)


def _kernel(x_hbm, gain_hbm, turn_hbm, base_hbm, wk, wv, wq, wo, out, x_s, gain_s, turn_s, base_s, a_s, w_s, k_s, v_s, q_s, seen_s, mix_s, top_s, cos_s,
            sin_s, in_sem, w_sem, send_sem, k_sem, v_sem, out_sem):
    me = lax.axis_index("sp")
    core = lax.rem(me, 2)
    chip = lax.div(me, 2)
    z = lax.rem(chip, 4)
    line = lax.div(chip, 4)
    y = lax.rem(line, 2)
    x = lax.div(line, 2)

    lines = {"o": line, "y": 2 * x + 1 - y, "x": 2 * (1 - x) + y, "d": 2 * (1 - x) + 1 - y}
    near, two, far = z + 1 - 2 * lax.rem(z, 2), lax.rem(z + 2, 4), 3 - z
    mid = lax.rem(lax.div(z + 1, 2), 2)
    places = [z, near, two + mid * (far - two), far + mid * (two - far)]

    def block(name, at, c=None):
        return (lines[name] * 4 + places[at]) * 2 + (core if c is None else c)

    other = me + 1 - 2 * core
    peers = {"p": other, "y": block("y", 0), "x": block("x", 0), 1: block("o", 1), 2: block("o", 2), 3: block("o", 3)}

    def copy(kind, b, to, n):
        ref = (k_s if kind == "k" else v_s).at[b]
        return pltpu.make_async_remote_copy(src_ref=ref, dst_ref=ref, send_sem=send_sem.at[n % 2],
                                            recv_sem=(k_sem if kind == "k" else v_sem).at[b],
                                            device_id=(0, to), device_id_type=MESH)

    sent = [0]

    def send(kind, b, *to):
        for t in to:
            copy(kind, b, peers[t], sent[0]).start()
            sent[0] += 1

    def arrived(kind, b):
        copy(kind, b, other, 0).wait_recv()

    def relay(kind, name, at, *to):
        b = block(name, at)
        arrived(kind, b)
        send(kind, b, *to)

    def fetch(c):
        src = wk if c == 0 else wv if c == 1 else wq.at[:, pl.ds((c - 2) * 256, 256)] if c < 18 else wo.at[:, pl.ds((c - 18) * 256, 256)]
        return pltpu.make_async_copy(src, w_s.at[c % SLOTS], w_sem.at[c % SLOTS])

    def more(c):
        for n in (c, c + 1):
            if n < CHUNKS:
                fetch(n).start()

    def landed(slot):
        pltpu.make_async_copy(wk, w_s.at[slot], w_sem.at[slot]).wait()

    x_copy = pltpu.make_async_copy(x_hbm, x_s, in_sem.at[0])
    gain_copy = pltpu.make_async_copy(gain_hbm, gain_s, in_sem.at[1])
    turn_copy = pltpu.make_async_copy(turn_hbm, turn_s, in_sem.at[2])
    base_copy = pltpu.make_async_copy(base_hbm.at[me], base_s, in_sem.at[3])
    x_copy.start()
    gain_copy.start()
    turn_copy.start()
    base_copy.start()
    fetch(0).start()
    fetch(1).start()

    barrier = pltpu.get_barrier_semaphore()
    for t in peers.values():
        pl.semaphore_signal(barrier, inc=1, device_id=(0, t), device_id_type=MESH)

    turn_copy.wait()
    base_copy.wait()
    near_cos, near_sin, far_cos, far_sin = turn_s[0], turn_s[1], base_s[0:1, :], base_s[1:2, :]
    cos_s[...] = near_cos * far_cos - near_sin * far_sin
    sin_s[...] = near_sin * far_cos + near_cos * far_sin

    x_copy.wait()
    gain_copy.wait()
    for c in range(2, 2 + DEPTH):
        fetch(c).start()

    gain = gain_s[...].reshape(1, D).astype(jnp.float32)
    for r in range(OWN // 16):
        rows = slice(r * 16, (r + 1) * 16)
        wide = x_s[rows, :].astype(jnp.float32)
        scale = lax.rsqrt(jnp.mean(wide * wide, -1, keepdims=True) + 1e-6)
        a_s[rows, :] = (wide * scale * gain).astype(jnp.bfloat16)

    def projected(slot):
        return _dot(a_s[...], w_s[slot]).astype(jnp.bfloat16).astype(jnp.float32)

    def turned(t):
        a, b = t[:, :HALF], t[:, HALF:]
        cos, sin = cos_s[...], sin_s[...]
        return a * cos - b * sin, b * cos + a * sin

    landed(0)
    landed(1)
    first, second = turned(projected(0))
    values = projected(1)
    k_s[me, :, :HALF] = first.astype(jnp.bfloat16)
    k_s[me, :, HALF:] = second.astype(jnp.bfloat16)
    v_s[me] = values.T.astype(jnp.bfloat16)

    pl.semaphore_wait(barrier, len(peers))
    send("k", me, 1, "y")
    send("v", me, 1, "x")
    send("k", me, "p", "x", 2)
    send("v", me, "p", "y", 2)
    send("k", me, 3)
    send("v", me, 3)

    def own_line(at):
        relay("k", "o", at, "y", "x", "p")
        relay("v", "o", at, "x", "y", "p")

    def across(at):
        relay("k", "y", at, "x", "p")
        relay("v", "x", at, "y", "p")

    def back(at):
        relay("v", "y", at, "p")
        relay("k", "x", at, "p")

    def corner(at):
        relay("k", "d", at, "p")
        relay("v", "d", at, "p")

    def from_other(*which):
        for name, at in which:
            b = block(name, at, 1 - core)
            arrived("k", b)
            arrived("v", b)

    events = {
        2: [(across, 0)],
        3: [(own_line, 1), (back, 0)],
        4: [(corner, 0)],
        5: [(across, 1)],
        6: [(back, 1)],
        7: [(own_line, 2), (from_other, ("o", 0), ("o", 1))],
    }
    for j in range(0, HEADS, 2):
        landed(j + 2)
        landed(j + 3)
        more(j + 2 + DEPTH)
        both = [projected(j + 2), projected(j + 3)]
        for n in range(2):
            first, second = turned(both[n])
            q_s[j + n, :HALF, :] = first.T.astype(jnp.bfloat16)
            q_s[j + n, HALF:, :] = second.T.astype(jnp.bfloat16)
        for f, *args in events.get(j // 2, ()):
            f(*args)

    def attend(start, masked):
        keys = k_s[pl.ds(start, 4)].reshape(512, HEAD)
        values = jnp.concatenate([v_s[start + i] for i in range(4)], axis=1)
        values = jnp.concatenate([values, jnp.ones((8, 512), jnp.bfloat16)], axis=0)

        def scores(i):
            return _dot(keys, jnp.concatenate([q_s[2 * i], q_s[2 * i + 1]], axis=1))

        if masked:
            place = lax.rem(z, 2) * 256 + core * OWN + lax.rem(lax.broadcasted_iota(jnp.int32, (512, 256), 1), OWN)
            ok = lax.broadcasted_iota(jnp.int32, (512, 256), 0) <= place
        s = scores(0)
        for i in range(STRIPS):
            then = scores(i + 1) if i + 1 < STRIPS else None
            if masked:
                s = jnp.where(ok, s, HIDDEN)
                top = s.max(axis=0, keepdims=True)
                p = jnp.exp2((s - top) * E).astype(jnp.bfloat16)
                mix_s[i] = _dot(values, p)
            else:
                old = top_s[i : i + 1, :]
                top = jnp.maximum(old, s.max(axis=0, keepdims=True))
                p = jnp.exp2((s - top) * E).astype(jnp.bfloat16)
                mix_s[i] = mix_s[i] * jnp.exp2((old - top) * E) + _dot(values, p)
            top_s[i : i + 1, :] = top
            s = then

    half = lax.div(z, 2)
    more(HEADS + 2 + DEPTH)
    attend(line * 8 + half * 4, True)

    for n, (name, h, calls) in enumerate((
        ("y", half, [(corner, 1), (from_other, ("y", 0), ("y", 1))]),
        ("x", half, [(own_line, 3), (across, 2), (from_other, ("x", 0), ("x", 1))]),
        ("d", half, [(back, 2), (from_other, ("d", 0), ("d", 1))]),
        ("o", 1 - half, [(across, 3), (from_other, ("o", 2), ("o", 3))]),
        ("y", 1 - half, [(back, 3), (corner, 2), (from_other, ("y", 2), ("y", 3))]),
        ("x", 1 - half, [(corner, 3), (from_other, ("x", 2), ("x", 3))]),
        ("d", 1 - half, [(from_other, ("d", 2), ("d", 3))]),
    )):
        more(HEADS + 2 + DEPTH + 2 * (n + 1))
        for f, *args in calls:
            f(*args)
        start = lines[name] * 2 + h

        @pl.when(start < line * 2 + half)
        def _(start=start):
            attend(start * 4, False)

    for i in range(STRIPS):
        done = mix_s[i, :HEAD, :] * (1 / mix_s[i, HEAD : HEAD + 1, :])
        for n in range(2):
            seen_s[:, (2 * i + n) * HEAD : (2 * i + n + 1) * HEAD] = done[:, n * OWN : (n + 1) * OWN].T.astype(jnp.bfloat16)

    def put(i):
        cols = pl.ds(pl.multiple_of(i * 512, 512), 512)
        return pltpu.make_async_copy(a_s.at[:, cols], out.at[:, cols], out_sem.at[i])

    def project(i, _):
        for n in range(2):
            slot = lax.rem(2 * i + n + 18, SLOTS)
            landed(slot)
        for n in range(2):
            slot = lax.rem(2 * i + n + 18, SLOTS)
            cols = pl.ds(pl.multiple_of((2 * i + n) * 256, 256), 256)
            a_s[:, cols] = (x_s[:, cols].astype(jnp.float32) + _dot(seen_s[...], w_s[slot])).astype(jnp.bfloat16)
        put(i).start()

    lax.fori_loop(0, 8, project, None)
    assert sent[0] == SENDS
    for n in range(2):
        ref = k_s.at[pl.ds(0, SENDS // 2)]
        pltpu.make_async_copy(ref, ref, send_sem.at[n]).wait()
    for i in range(8):
        put(i).wait()


def solution(mesh):
    angle = np.float64(THETA) ** (-np.arange(HALF) / HALF)
    near, far = np.arange(OWN)[:, None] * angle, np.arange(32)[:, None] * OWN * angle
    near = np.stack([np.cos(near), np.sin(near)]).astype(np.float32)
    far = np.stack([np.cos(far), np.sin(far)], 1).astype(np.float32)

    def step(x, gain, wq, wk, wv, wo):
        bf16, f32 = jnp.bfloat16, jnp.float32
        return pl.pallas_call(
            _kernel,
            out_shape=jax.ShapeDtypeStruct((OWN, D), bf16),
            in_specs=[pl.BlockSpec(memory_space=pl.ANY)] * 8,
            out_specs=pl.BlockSpec(memory_space=pl.ANY),
            scratch_shapes=[
                pltpu.VMEM((OWN, D), bf16),
                pltpu.VMEM((D,), bf16),
                pltpu.VMEM((2, OWN, HALF), f32),
                pltpu.VMEM((2, HALF), f32),
                pltpu.VMEM((OWN, D), bf16),
                pltpu.VMEM((SLOTS, D, 256), bf16),
                pltpu.VMEM((32, OWN, HEAD), bf16),
                pltpu.VMEM((32, HEAD, OWN), bf16),
                pltpu.VMEM((HEADS, HEAD, OWN), bf16),
                pltpu.VMEM((OWN, D), bf16),
                pltpu.VMEM((STRIPS, HEAD + 8, 256), f32),
                pltpu.VMEM((STRIPS, 256), f32),
                pltpu.VMEM((OWN, HALF), f32),
                pltpu.VMEM((OWN, HALF), f32),
                pltpu.SemaphoreType.DMA((4,)),
                pltpu.SemaphoreType.DMA((SLOTS,)),
                pltpu.SemaphoreType.DMA((2,)),
                pltpu.SemaphoreType.DMA((32,)),
                pltpu.SemaphoreType.DMA((32,)),
                pltpu.SemaphoreType.DMA((8,)),
            ],
            compiler_params=pltpu.CompilerParams(collective_id=0, has_side_effects=True, vmem_limit_bytes=67043328),
        )(x, gain, jnp.asarray(near), jnp.asarray(far), wk, wv, wq, wo)

    tokens, whole = P(("dp", "sp"), None), P(None, None)
    return jax.shard_map(
        step,
        mesh=mesh,
        in_specs=(tokens, P(None), whole, whole, whole, whole),
        out_specs=tokens,
        check_vma=False,
    )
```

```python
import functools

import jax
import jax.numpy as jnp
import numpy as np
from jax import lax
from jax.experimental import pallas as pl
from jax.experimental.pallas import tpu as pltpu
from jax.sharding import PartitionSpec as P

HEAD = 256
HALF = 128
HEADS = 16
D = 4096
OWN = 128
THETA = 10000
LOG2E = 1.4426950408889634
E = HEAD**-0.5 * LOG2E
HIDDEN = -2e30
SLOTS = 18
CHUNKS = 34
DEPTH = 4
WIDE = 512
STRIPS = 4
SENDS = 62
MESH = pl.DeviceIdType.MESH


def _dot(a, b):
    return jnp.dot(a, b, preferred_element_type=jnp.float32)


def _kernel(x_hbm, gain_hbm, turn_hbm, base_hbm, wk, wv, wq, wo, out, x_s, gain_s, turn_s, base_s, a_s, w_s, k_s, v_s, q_s, seen_s, mix_s, top_s, cos_s,
            sin_s, in_sem, w_sem, send_sem, k_sem, v_sem):
    me = lax.axis_index("sp")
    core = lax.rem(me, 2)
    chip = lax.div(me, 2)
    z = lax.rem(chip, 4)
    line = lax.div(chip, 4)
    y = lax.rem(line, 2)
    x = lax.div(line, 2)

    lines = {"o": line, "y": 2 * x + 1 - y, "x": 2 * (1 - x) + y, "d": 2 * (1 - x) + 1 - y}
    near, two, far = z + 1 - 2 * lax.rem(z, 2), lax.rem(z + 2, 4), 3 - z
    mid = lax.rem(lax.div(z + 1, 2), 2)
    places = [z, near, two + mid * (far - two), far + mid * (two - far)]

    def block(name, at, c=None):
        return (lines[name] * 4 + places[at]) * 2 + (core if c is None else c)

    other = me + 1 - 2 * core
    peers = {"p": other, "y": block("y", 0), "x": block("x", 0), 1: block("o", 1), 2: block("o", 2), 3: block("o", 3)}

    def copy(kind, b, to, n):
        ref = (k_s if kind == "k" else v_s).at[b]
        return pltpu.make_async_remote_copy(src_ref=ref, dst_ref=ref, send_sem=send_sem.at[n % 2],
                                            recv_sem=(k_sem if kind == "k" else v_sem).at[b],
                                            device_id=(0, to), device_id_type=MESH)

    sent = [0]

    def send(kind, b, *to):
        for t in to:
            copy(kind, b, peers[t], sent[0]).start()
            sent[0] += 1

    def arrived(kind, b):
        copy(kind, b, other, 0).wait_recv()

    def relay(kind, name, at, *to):
        b = block(name, at)
        arrived(kind, b)
        send(kind, b, *to)

    def fetch(c):
        src = wk if c == 0 else wv if c == 1 else wq.at[:, pl.ds((c - 2) * 256, 256)] if c < 18 else wo.at[:, pl.ds((c - 18) * 256, 256)]
        return pltpu.make_async_copy(src, w_s.at[c % SLOTS], w_sem.at[c % SLOTS])

    def more(c):
        for n in (c, c + 1):
            if n < CHUNKS:
                fetch(n).start()

    def landed(slot):
        pltpu.make_async_copy(wk, w_s.at[slot], w_sem.at[slot]).wait()

    x_copy = pltpu.make_async_copy(x_hbm, x_s, in_sem.at[0])
    gain_copy = pltpu.make_async_copy(gain_hbm, gain_s, in_sem.at[1])
    turn_copy = pltpu.make_async_copy(turn_hbm, turn_s, in_sem.at[2])
    base_copy = pltpu.make_async_copy(base_hbm.at[me], base_s, in_sem.at[3])
    x_copy.start()
    gain_copy.start()
    turn_copy.start()
    base_copy.start()
    fetch(0).start()
    fetch(1).start()

    barrier = pltpu.get_barrier_semaphore()
    for t in peers.values():
        pl.semaphore_signal(barrier, inc=1, device_id=(0, t), device_id_type=MESH)

    turn_copy.wait()
    base_copy.wait()
    near_cos, near_sin, far_cos, far_sin = turn_s[0], turn_s[1], base_s[0:1, :], base_s[1:2, :]
    cos_s[...] = near_cos * far_cos - near_sin * far_sin
    sin_s[...] = near_sin * far_cos + near_cos * far_sin

    x_copy.wait()
    gain_copy.wait()
    for c in range(2, 2 + DEPTH):
        fetch(c).start()

    gain = gain_s[...].reshape(1, D).astype(jnp.float32)
    for r in range(OWN // 16):
        rows = slice(r * 16, (r + 1) * 16)
        wide = x_s[rows, :].astype(jnp.float32)
        scale = lax.rsqrt(jnp.mean(wide * wide, -1, keepdims=True) + 1e-6)
        a_s[rows, :] = (wide * scale * gain).astype(jnp.bfloat16)

    def projected(slot):
        return _dot(a_s[...], w_s[slot]).astype(jnp.bfloat16).astype(jnp.float32)

    def turned(t):
        a, b = t[:, :HALF], t[:, HALF:]
        cos, sin = cos_s[...], sin_s[...]
        return a * cos - b * sin, b * cos + a * sin

    landed(0)
    landed(1)
    first, second = turned(projected(0))
    values = projected(1)
    k_s[me, :, :HALF] = first.astype(jnp.bfloat16)
    k_s[me, :, HALF:] = second.astype(jnp.bfloat16)
    v_s[me] = values.T.astype(jnp.bfloat16)

    pl.semaphore_wait(barrier, len(peers))
    send("k", me, 1, "y")
    send("v", me, 1, "x")
    send("k", me, "p", "x", 2)
    send("v", me, "p", "y", 2)
    send("k", me, 3)
    send("v", me, 3)

    def own_line(at):
        relay("k", "o", at, "y", "x", "p")
        relay("v", "o", at, "x", "y", "p")

    def across(at):
        relay("k", "y", at, "x", "p")
        relay("v", "x", at, "y", "p")

    def back(at):
        relay("v", "y", at, "p")
        relay("k", "x", at, "p")

    def corner(at):
        relay("k", "d", at, "p")
        relay("v", "d", at, "p")

    def from_other(*which):
        for name, at in which:
            b = block(name, at, 1 - core)
            arrived("k", b)
            arrived("v", b)

    events = {
        2: [(across, 0)],
        3: [(own_line, 1), (back, 0)],
        4: [(corner, 0)],
        5: [(across, 1)],
        6: [(back, 1)],
        7: [(own_line, 2), (from_other, ("o", 0), ("o", 1))],
    }
    for j in range(0, HEADS, 2):
        landed(j + 2)
        landed(j + 3)
        more(j + 2 + DEPTH)
        both = [projected(j + 2), projected(j + 3)]
        for n in range(2):
            first, second = turned(both[n])
            q_s[j + n, :HALF, :] = first.T.astype(jnp.bfloat16)
            q_s[j + n, HALF:, :] = second.T.astype(jnp.bfloat16)
        for f, *args in events.get(j // 2, ()):
            f(*args)

    def attend(start, masked):
        keys = k_s[pl.ds(start, 4)].reshape(512, HEAD)
        values = jnp.concatenate([v_s[start + i] for i in range(4)], axis=1)
        values = jnp.concatenate([values, jnp.ones((8, 512), jnp.bfloat16)], axis=0)

        if masked:
            place = lax.rem(z, 2) * 256 + core * OWN + lax.rem(lax.broadcasted_iota(jnp.int32, (512, WIDE), 1), OWN)
            ok = lax.broadcasted_iota(jnp.int32, (512, WIDE), 0) <= place
        scores = [_dot(keys, jnp.concatenate([q_s[4 * i + n] for n in range(4)], axis=1)) for i in range(STRIPS)]
        ready = []

        def gather(i):
            cols, p, keep = ready[i]
            new = _dot(values, p)
            mix_s[:, cols] = new if keep is None else mix_s[:, cols] * keep + new

        for i, s in enumerate(scores):
            cols = slice(i * WIDE, (i + 1) * WIDE)
            keep = None
            if masked:
                s = jnp.where(ok, s, HIDDEN)
                top = s.max(axis=0, keepdims=True)
            else:
                old = top_s[:, cols]
                top = jnp.maximum(old, s.max(axis=0, keepdims=True))
                keep = jnp.exp2((old - top) * E)
            ready.append((cols, jnp.exp2((s - top) * E).astype(jnp.bfloat16), keep))
            top_s[:, cols] = top
            if i:
                gather(i - 1)
        gather(STRIPS - 1)

    half = lax.div(z, 2)
    more(HEADS + 2 + DEPTH)
    attend(line * 8 + half * 4, True)

    for n, (name, h, calls) in enumerate((
        ("y", half, [(corner, 1), (from_other, ("y", 0), ("y", 1))]),
        ("x", half, [(own_line, 3), (across, 2), (from_other, ("x", 0), ("x", 1))]),
        ("d", half, [(back, 2), (from_other, ("d", 0), ("d", 1))]),
        ("o", 1 - half, [(across, 3), (from_other, ("o", 2), ("o", 3))]),
        ("y", 1 - half, [(back, 3), (corner, 2), (from_other, ("y", 2), ("y", 3))]),
        ("x", 1 - half, [(corner, 3), (from_other, ("x", 2), ("x", 3))]),
        ("d", 1 - half, [(from_other, ("d", 2), ("d", 3))]),
    )):
        more(HEADS + 2 + DEPTH + 2 * (n + 1))
        for f, *args in calls:
            f(*args)
        start = lines[name] * 2 + h

        @pl.when(start < line * 2 + half)
        def _(start=start):
            attend(start * 4, False)

    for h in range(HEADS):
        cols = slice(h * OWN, (h + 1) * OWN)
        done = mix_s[:HEAD, cols] * (1 / mix_s[HEAD : HEAD + 1, cols])
        seen_s[:, h * HEAD : (h + 1) * HEAD] = done.T.astype(jnp.bfloat16)

    def project(i, _):
        for n in range(2):
            slot = lax.rem(2 * i + n + 18, SLOTS)
            landed(slot)
        for n in range(2):
            slot = lax.rem(2 * i + n + 18, SLOTS)
            cols = pl.ds(pl.multiple_of((2 * i + n) * 256, 256), 256)
            out[:, cols] = (x_s[:, cols].astype(jnp.float32) + _dot(seen_s[...], w_s[slot])).astype(jnp.bfloat16)

    lax.fori_loop(0, 8, project, None)
    assert sent[0] == SENDS
    for n in range(2):
        ref = k_s.at[pl.ds(0, SENDS // 2)]
        pltpu.make_async_copy(ref, ref, send_sem.at[n]).wait()


def solution(mesh):
    angle = np.float64(THETA) ** (-np.arange(HALF) / HALF)
    near, far = np.arange(OWN)[:, None] * angle, np.arange(32)[:, None] * OWN * angle
    near = np.stack([np.cos(near), np.sin(near)]).astype(np.float32)
    far = np.stack([np.cos(far), np.sin(far)], 1).astype(np.float32)

    def step(x, gain, wq, wk, wv, wo):
        bf16, f32 = jnp.bfloat16, jnp.float32
        return pl.pallas_call(
            _kernel,
            out_shape=pltpu.VMEM((OWN, D), bf16),
            in_specs=[pl.BlockSpec(memory_space=pl.ANY)] * 8,
            out_specs=pl.BlockSpec(memory_space=pltpu.VMEM),
            scratch_shapes=[
                pltpu.VMEM((OWN, D), bf16),
                pltpu.VMEM((D,), bf16),
                pltpu.VMEM((2, OWN, HALF), f32),
                pltpu.VMEM((2, HALF), f32),
                pltpu.VMEM((OWN, D), bf16),
                pltpu.VMEM((SLOTS, D, 256), bf16),
                pltpu.VMEM((32, OWN, HEAD), bf16),
                pltpu.VMEM((32, HEAD, OWN), bf16),
                pltpu.VMEM((HEADS, HEAD, OWN), bf16),
                pltpu.VMEM((OWN, D), bf16),
                pltpu.VMEM((HEAD + 8, STRIPS * WIDE), f32),
                pltpu.VMEM((1, STRIPS * WIDE), f32),
                pltpu.VMEM((OWN, HALF), f32),
                pltpu.VMEM((OWN, HALF), f32),
                pltpu.SemaphoreType.DMA((4,)),
                pltpu.SemaphoreType.DMA((SLOTS,)),
                pltpu.SemaphoreType.DMA((2,)),
                pltpu.SemaphoreType.DMA((32,)),
                pltpu.SemaphoreType.DMA((32,)),
            ],
            compiler_params=pltpu.CompilerParams(collective_id=0, has_side_effects=True, vmem_limit_bytes=62 * 2**20),
        )(x, gain, jnp.asarray(near), jnp.asarray(far), wk, wv, wq, wo)

    tokens, whole = P(("dp", "sp"), None), P(None, None)
    return jax.shard_map(
        step,
        mesh=mesh,
        in_specs=(tokens, P(None), whole, whole, whole, whole),
        out_specs=tokens,
        check_vma=False,
    )
```
